16 devices in a mesh: dp: 2 (over z), tp: 8 (over y, x, core).
Axes of the slice: x: 2, y: 2, z: 2, core: 2. Of those that a mesh axis runs over, the one named last changes fastest.
Arguments:
- hidden: bfloat16 [6, 512, 960], P('dp')
- norm_w: bfloat16 [960], replicated
- embed_table: bfloat16 [49152, 960], P('tp')
- labels: int32 [6, 512], P('dp')
- loss_mask: int32 [6, 512], P('dp')
Outputs:
- output 1: float32 [], replicated
- output 2: bfloat16 [6, 512, 960], P('dp')
- output 3: float32 [960], replicated
- output 4: float32 [49152, 960], P('tp')
All inputs are finite; a program needn't handle non-finite values.
Results may differ from the reference program's by a relative error of at most 0.001.
Values sent between devices are 32-bit elements.
A program may use at most 1 GiB of HBM per device.

```python
import math
import jax
import jax.numpy as jnp
from jax import lax

BATCH_ROWS = 6
SEQ_LEN = 512
MODEL_DIM = 960
VOCAB_SIZE = 49152
TOKEN_BLOCK = 128
SOFT_CAP = 30.0


def draw_labels(root_key):
    key_pick, key_common, key_any = jax.random.split(root_key, 3)
    label_shape = (BATCH_ROWS, SEQ_LEN)
    pick_val = jax.random.randint(key_pick, label_shape, 0, 4)
    common_id = jax.random.randint(key_common, label_shape, 0, VOCAB_SIZE // 32)
    any_id = jax.random.randint(key_any, label_shape, 0, VOCAB_SIZE)
    return jnp.where(pick_val == 0, any_id, common_id).astype(jnp.int32)


def draw_mask(root_key):
    key_rate, key_roll = jax.random.split(root_key, 2)
    drop_pct = jax.random.randint(key_rate, (BATCH_ROWS, 1), 5, 40)
    roll_val = jax.random.randint(key_roll, (BATCH_ROWS, SEQ_LEN), 0, 100)
    return (roll_val >= drop_pct).astype(jnp.int32)


def norm_apply(hid_rows, gain32):
    h32 = hid_rows.astype(jnp.float32)
    inv_rms = lax.rsqrt(jnp.mean(h32 * h32, axis=-1, keepdims=True) + 1e-6)
    return h32 * inv_rms * (1.0 + gain32)


def setup_inputs(seed: int = 0) -> dict:
    root_key = jax.random.key(seed)
    key_noise, key_gain, key_table, key_str, key_lab, key_mask, key_top = jax.random.split(root_key, 7)
    table_scale = 3.0 / math.sqrt(MODEL_DIM)
    table32 = jax.random.normal(key_table, (VOCAB_SIZE, MODEL_DIM), jnp.float32) * table_scale
    labels = draw_labels(key_lab)
    top_str = jax.random.uniform(key_top, (), jnp.float32, minval=3.0, maxval=6.5)
    strength = jax.random.uniform(key_str, (BATCH_ROWS, SEQ_LEN, 1), jnp.float32) * top_str
    noise_val = jax.random.normal(key_noise, (BATCH_ROWS, SEQ_LEN, MODEL_DIM), jnp.float32)
    hidden = noise_val + strength * jnp.take(table32, labels, axis=0)
    gain_vec = 0.3 * jax.random.normal(key_gain, (MODEL_DIM,), jnp.float32)
    return {'hidden': hidden.astype(jnp.bfloat16), 'norm_w': gain_vec.astype(jnp.bfloat16), 'embed_table': table32.astype(jnp.bfloat16), 'labels': labels, 'loss_mask': draw_mask(key_mask)}


def reference(hidden, norm_w, embed_table, labels, loss_mask):
    tokens = BATCH_ROWS * SEQ_LEN
    n_blocks = tokens // TOKEN_BLOCK
    hid_blocks = hidden.reshape(n_blocks, TOKEN_BLOCK, MODEL_DIM)
    lab_blocks = labels.reshape(n_blocks, TOKEN_BLOCK)
    mask_blocks = loss_mask.reshape(n_blocks, TOKEN_BLOCK).astype(jnp.float32)
    tok_count = jnp.maximum(jnp.sum(mask_blocks), 1.0)
    gain32 = norm_w.astype(jnp.float32)
    vocab_ids = jnp.arange(VOCAB_SIZE, dtype=jnp.int32)

    def block_step(carry_in, block_in):
        loss_sum, grad_gain, grad_table = carry_in
        hid_rows, lab_rows, mask_rows = block_in
        normed, norm_back = jax.vjp(norm_apply, hid_rows, gain32)
        normed_bf = normed.astype(jnp.bfloat16)
        logits = jnp.dot(normed_bf, embed_table.T, preferred_element_type=jnp.float32)
        capped = SOFT_CAP * jnp.tanh(logits / SOFT_CAP)
        row_max = jnp.max(capped, axis=-1, keepdims=True)
        exp_shift = jnp.exp(capped - row_max)
        row_sum = jnp.sum(exp_shift, axis=-1, keepdims=True)
        onehot = vocab_ids[None, :] == lab_rows[:, None]
        picked = jnp.sum(jnp.where(onehot, capped, 0.0), axis=-1)
        tok_loss = jnp.log(row_sum[:, 0]) + row_max[:, 0] - picked
        tok_scale = mask_rows / tok_count
        cap_ratio = capped / SOFT_CAP
        grad_logit = ((exp_shift / row_sum - onehot.astype(jnp.float32)) * tok_scale[:, None] * (1.0 - cap_ratio * cap_ratio)).astype(jnp.bfloat16)
        grad_x = jnp.dot(grad_logit, embed_table, preferred_element_type=jnp.float32)
        grad_rows, grad_g = norm_back(grad_x)
        table_part = jnp.dot(grad_logit.T, normed_bf, preferred_element_type=jnp.float32)
        new_carry = (loss_sum + jnp.sum(mask_rows * tok_loss), grad_gain + grad_g, grad_table + table_part)
        return new_carry, grad_rows

    init_carry = (jnp.zeros((), jnp.float32), jnp.zeros((MODEL_DIM,), jnp.float32), jnp.zeros((VOCAB_SIZE, MODEL_DIM), jnp.float32))
    final_carry, grad_rows = lax.scan(block_step, init_carry, (hid_blocks, lab_blocks, mask_blocks))
    loss_sum, grad_gain, grad_table = final_carry
    return loss_sum / tok_count, grad_rows.reshape(BATCH_ROWS, SEQ_LEN, MODEL_DIM), grad_gain, grad_table
```

```python
import functools

import jax
import jax.numpy as jnp
from jax import lax
from jax.experimental import pallas as pl
from jax.experimental.pallas import tpu as pltpu
from jax.sharding import PartitionSpec as P

SOFT_CAP = 30.0
EXP2_SCALE = 30.0 * 1.4426950408889634
VMEM = pltpu.VMEM
PARAMS = pltpu.CompilerParams(vmem_limit_bytes=62 * 1024 * 1024)


def logits_kernel(x_ref, et_ref, t_ref, z_ref, *, sub):
    rows, cols = t_ref.shape
    here = pl.ds(pl.multiple_of(pl.program_id(1) * rows, rows), rows)

    @pl.when(pl.program_id(0) == 0)
    def _():
        z_ref[here, :] = jnp.zeros((rows, 128), jnp.float32)

    acc = jnp.zeros((rows, 128), jnp.float32)
    for s in range(cols // sub):
        z = jnp.dot(x_ref[...], et_ref[:, s * sub:(s + 1) * sub], preferred_element_type=jnp.float32)
        t = jnp.tanh(z * (1.0 / SOFT_CAP))
        t_ref[:, s * sub:(s + 1) * sub] = t
        e = jnp.exp2(t * EXP2_SCALE)
        for c in range(sub // 128):
            acc = acc + e[:, c * 128:(c + 1) * 128]
    z_ref[here, :] += acc


def logits_call(x, et, vb=1024, sub=1024, tb=512):
    tokens, dim = x.shape
    vocab = et.shape[1]
    return pl.pallas_call(
        functools.partial(logits_kernel, sub=sub),
        grid=(vocab // vb, tokens // tb),
        in_specs=[pl.BlockSpec((tb, dim), lambda v, t: (t, 0)), pl.BlockSpec((dim, vb), lambda v, t: (0, v))],
        out_specs=[pl.BlockSpec((tb, vb), lambda v, t: (t, v)), pl.BlockSpec((tokens, 128), lambda v, t: (0, 0))],
        out_shape=[jax.ShapeDtypeStruct((tokens, vocab), jnp.float32), jax.ShapeDtypeStruct((tokens, 128), jnp.float32)],
        compiler_params=PARAMS,
        cost_estimate=pl.CostEstimate(flops=2 * tokens * vocab * dim, bytes_accessed=4 * tokens * vocab, transcendentals=0),
        name="logits",
    )(x, et)


def grad_of(t, cz, a, lab, v0):
    e = jnp.exp2(t * EXP2_SCALE)
    vid = lax.broadcasted_iota(jnp.int32, t.shape, 1) + v0
    return ((e * cz - jnp.where(vid == lab, a, 0.0)) * (1.0 - t * t)).astype(jnp.bfloat16)


def gx_kernel(t_ref, et_ref, cz_ref, a_ref, lab_ref, g_ref, gx_ref, pick_ref, *, sub):
    vb = pl.program_id(1)

    @pl.when(vb == 0)
    def _():
        gx_ref[...] = jnp.zeros_like(gx_ref)
        pick_ref[...] = jnp.zeros_like(pick_ref)

    rows, cols = t_ref.shape
    pick = jnp.zeros((rows, 128), jnp.float32)
    for s in range(cols // sub):
        sl = slice(s * sub, (s + 1) * sub)
        v0 = vb * cols + s * sub
        t = t_ref[:, sl]
        g_ref[:, sl] = grad_of(t, cz_ref[...], a_ref[...], lab_ref[...], v0)
        hit = lax.broadcasted_iota(jnp.int32, t.shape, 1) + v0 == lab_ref[...]
        p = jnp.where(hit, t, 0.0)
        for c in range(sub // 128):
            pick = pick + p[:, c * 128:(c + 1) * 128]
    pick_ref[...] += pick
    gx_ref[...] += lax.dot_general(et_ref[...], g_ref[...], (((1,), (1,)), ((), ())), preferred_element_type=jnp.float32)


def gx_call(t, et, cz, a, lab, vb=1024, sub=256, tb=512):
    tokens, vocab = t.shape
    dim = et.shape[0]
    return pl.pallas_call(
        functools.partial(gx_kernel, sub=sub),
        grid=(tokens // tb, vocab // vb),
        in_specs=[pl.BlockSpec((tb, vb), lambda t, v: (t, v)), pl.BlockSpec((dim, vb), lambda t, v: (0, v))]
        + [pl.BlockSpec((tb, 1), lambda t, v: (t, 0))] * 3,
        out_specs=[pl.BlockSpec((tb, vb), lambda t, v: (t, v)), pl.BlockSpec((dim, tb), lambda t, v: (0, t)), pl.BlockSpec((tb, 128), lambda t, v: (t, 0))],
        out_shape=[jax.ShapeDtypeStruct((tokens, vocab), jnp.bfloat16), jax.ShapeDtypeStruct((dim, tokens), jnp.float32), jax.ShapeDtypeStruct((tokens, 128), jnp.float32)],
        compiler_params=PARAMS,
        cost_estimate=pl.CostEstimate(flops=2 * tokens * vocab * dim, bytes_accessed=6 * tokens * vocab, transcendentals=0),
        name="grad_x",
    )(t, et, cz, a, lab)


def table_kernel(go_ref, t_ref, xo_ref, xt_ref, cz_ref, a_ref, lab_ref, de_ref, gs_ref, *, sub):
    rows, cols = t_ref.shape
    v0 = pl.program_id(0) * cols
    for s in range(rows // sub):
        sl = slice(s * sub, (s + 1) * sub)
        gs_ref[sl, :] = grad_of(t_ref[sl, :], cz_ref[sl, :], a_ref[sl, :], lab_ref[sl, :], v0)
    own = jnp.dot(xo_ref[...], go_ref[...], preferred_element_type=jnp.float32)
    de_ref[...] = own + jnp.dot(xt_ref[...], gs_ref[...], preferred_element_type=jnp.float32)


def table_call(g_own, t_other, xt_own, xt_other, cz, a, lab, vb=512, sub=64):
    tokens, vocab = t_other.shape
    dim = xt_own.shape[0]
    whole = pl.BlockSpec(memory_space=VMEM)
    return pl.pallas_call(
        functools.partial(table_kernel, sub=sub),
        grid=(vocab // vb,),
        in_specs=[pl.BlockSpec((tokens, vb), lambda v: (0, v)), pl.BlockSpec((tokens, vb), lambda v: (0, v))] + [whole] * 5,
        out_specs=pl.BlockSpec((dim, vb), lambda v: (0, v)),
        out_shape=jax.ShapeDtypeStruct((dim, vocab), jnp.float32),
        scratch_shapes=[pltpu.VMEM((tokens, vb), jnp.bfloat16)],
        compiler_params=PARAMS,
        cost_estimate=pl.CostEstimate(flops=4 * tokens * vocab * dim, bytes_accessed=10 * tokens * vocab, transcendentals=0),
        name="grad_table",
    )(g_own, t_other, xt_own, xt_other, cz, a, lab)


def norm_kernel(h_ref, gain_ref, xf_ref, xb_ref, xr_ref):
    h = h_ref[0].astype(jnp.float32)
    inv = lax.rsqrt(jnp.mean(h * h, axis=0, keepdims=True) + 1e-6)
    xb = (h * inv * gain_ref[...]).astype(jnp.bfloat16)
    xb_ref[...] = xb
    xf_ref[...] = xb.astype(jnp.float32)
    xr_ref[...] = xb.T


def norm_call(ht, gain):
    batch, dim, seq = ht.shape
    return pl.pallas_call(
        norm_kernel,
        grid=(batch,),
        in_specs=[pl.BlockSpec((1, dim, seq), lambda b: (b, 0, 0)), pl.BlockSpec((dim, 1), lambda b: (0, 0))],
        out_specs=[pl.BlockSpec((dim, seq), lambda b: (0, b)), pl.BlockSpec((dim, seq), lambda b: (0, b)), pl.BlockSpec((seq, dim), lambda b: (b, 0))],
        out_shape=[jax.ShapeDtypeStruct((dim, batch * seq), jnp.float32), jax.ShapeDtypeStruct((dim, batch * seq), jnp.bfloat16), jax.ShapeDtypeStruct((batch * seq, dim), jnp.bfloat16)],
        compiler_params=PARAMS,
        name="norm",
    )(ht, gain)


def unpack_kernel(xf_ref, xb_ref, xr_ref):
    xb = xf_ref[...].astype(jnp.bfloat16)
    xb_ref[...] = xb
    xr_ref[...] = xb.T


def unpack_call(xf, seq=512):
    dim, tokens = xf.shape
    return pl.pallas_call(
        unpack_kernel,
        grid=(tokens // seq,),
        in_specs=[pl.BlockSpec((dim, seq), lambda b: (0, b))],
        out_specs=[pl.BlockSpec((dim, seq), lambda b: (0, b)), pl.BlockSpec((seq, dim), lambda b: (b, 0))],
        out_shape=[jax.ShapeDtypeStruct((dim, tokens), jnp.bfloat16), jax.ShapeDtypeStruct((tokens, dim), jnp.bfloat16)],
        compiler_params=PARAMS,
        name="unpack",
    )(xf)


def solution(mesh):
    n_tp = mesh.shape['tp']

    def local_step(hidden, norm_w, embed_table, labels, loss_mask):
        batch, seq, dim = hidden.shape
        vocab_local = embed_table.shape[0]
        tokens = batch * seq
        shard = dim // n_tp
        tp = lax.axis_index('tp')
        et = embed_table.T
        gain = (1.0 + norm_w.astype(jnp.float32))[:, None]
        ht = hidden.transpose(0, 2, 1).astype(jnp.float32)
        inv = lax.rsqrt(jnp.mean(ht * ht, axis=1, keepdims=True) + 1e-6)
        xf, xt, xr = norm_call(hidden.transpose(0, 2, 1), gain)
        mine = lax.dynamic_slice_in_dim(xf, tp * shard, shard, 0)
        other = lax.ppermute(mine, 'dp', [(0, 1), (1, 0)])
        xt_other, xr_other = unpack_call(lax.all_gather(other, 'tp', axis=0, tiled=True))
        lm = jnp.stack([labels.reshape(tokens), loss_mask.reshape(tokens)])
        lm_other = lax.ppermute(lm, 'dp', [(0, 1), (1, 0)])
        mask = lm[1].astype(jnp.float32)
        mask_other = lm_other[1].astype(jnp.float32)
        count = jnp.maximum(jnp.sum(mask) + jnp.sum(mask_other), 1.0)

        t_own, z_own = logits_call(xr, et)
        z_own = lax.psum(jnp.sum(z_own, axis=1), 'tp')
        a_own = mask / count
        g_own, gx, pick = gx_call(t_own, et, (a_own / z_own)[:, None], a_own[:, None], (lm[0] - tp * vocab_local)[:, None])
        t_other, z_other = logits_call(xr_other, et)
        gx = lax.psum(gx, 'tp')
        z_other = lax.psum(jnp.sum(z_other, axis=1), 'tp')
        a_other = mask_other / count
        grad_table = table_call(g_own, t_other, xt, xt_other, (a_other / z_other)[:, None], a_other[:, None], (lm_other[0] - tp * vocab_local)[:, None])

        picked = lax.psum(jnp.sum(pick, axis=1), 'tp') * SOFT_CAP
        loss = jnp.sum(mask * (jnp.log(z_own) - picked))
        gx3 = gx.reshape(dim, batch, seq).transpose(1, 0, 2)
        gg = gx3 * gain
        dot = jnp.sum(gg * ht, axis=1, keepdims=True)
        dh = (gg * inv - ht * (inv * inv * inv / dim) * dot).astype(hidden.dtype)
        dw = jnp.sum(gx3 * ht * inv, axis=(0, 2))
        loss, dw = lax.psum((loss, dw), 'dp')
        return loss / count, dh.transpose(0, 2, 1), dw, grad_table.T

    return jax.shard_map(local_step, mesh=mesh, in_specs=(P('dp', None, None), P(None), P('tp', None), P('dp', None), P('dp', None)), out_specs=(P(), P('dp', None, None), P(None), P('tp', None)), check_vma=False)
```
